32 devices in a mesh: groups: 2 (over y), tensor: 4 (over z), dp: 2 (over x), pipe: 2 (over core).
Axes of the slice: x: 2, y: 2, z: 4, core: 2. Of those that a mesh axis runs over, the one named last changes fastest.
Arguments:
- activations: bfloat16 [2, 2048, 8192], P('pipe', ('groups', 'dp'), 'tensor'), parts along dimension 1, may hold values from -6 to 6
- cotangents: bfloat16 [2, 2048, 8192], P('pipe', ('groups', 'dp', 'tensor')), parts along dimension 1, may hold values from -6 to 6
- out_weight: bfloat16 [2, 8192, 8192], P('pipe', 'tensor', 'dp'), may hold values from -0.0625 to 0.0625
- in_sketch: bfloat16 [2, 64, 8192], P('pipe', None, 'tensor'), may hold values from -0.25 to 0.25
- out_sketch: bfloat16 [2, 64, 8192], P('pipe'), may hold values from -0.25 to 0.25
- queries: bfloat16 [2, 512, 4096], P('pipe', 'dp', 'tensor'), may hold values from -0.09375 to 0.09375
- lengths: int32 [8], P('groups'), parts along dimension 0, may hold values from 128 to 256
- store_order: int32 [8], P('groups'), parts along dimension 0, may hold values from 0 to 3, each once
Outputs:
- act_grads: bfloat16 [2, 2048, 8192], P('pipe', ('groups', 'dp'), 'tensor'), parts along dimension 1
- sketch_store: bfloat16 [2, 8, 4096], P('pipe', ('groups', 'dp'), 'tensor'), parts along dimension 1
- scores: float32 [8, 512], P('groups', ('dp', 'tensor', 'pipe')), parts along dimension 0
The draws below stay inside these ranges and needn't reach their ends.
There are 2 independent parts, one for each index of `groups`. The reference program is written for one: setup_inputs(seed, part) draws one part's arguments, and reference() takes and returns one part's arrays. A program takes and returns all parts, laid end to end along the dimension named above; an argument that names none is the same for every part. Nothing has to cross between parts.
Inputs may be any that keep to these rules, and one draw needn't show every extreme that they name: Example e's loss covers its first lengths[e] tokens. `store_order`: a permutation of the 4 examples.
All inputs are finite; a program needn't handle non-finite values.
Results may differ from the reference program's by a relative error of at most 0.0049.
Values may be sent and summed in bfloat16 or wider, within the bound.
No kernel may reach another device: no remote copies, remote signals or barrier semaphores. Data moves between devices by JAX's collectives and lax.ppermute only.
A program may use at most 128 MiB of HBM per device.

```python
import jax
import jax.numpy as jnp
from jax import lax

D = 8192
RANK = 64
LAY_DEV = 1
LEN = 256
TOKENS = 1024
EXAMPLES = 4
QUERIES = 512
LAYERS = 2
FEAT = 4096
N_PIPE = 2


def touch_ends(values, stream_key, smallest, largest):
    longest = values.shape.index(max(values.shape))
    spots = []
    for shift in (0, 1):
        where = [jax.random.randint(jax.random.fold_in(stream_key, axis), (), 0, length) for axis, length in enumerate(values.shape)]
        where[longest] = (where[longest] + shift) % values.shape[longest]
        spots.append(tuple(where))
    return values.at[spots[0]].set(smallest).at[spots[1]].set(largest)


def with_spikes(values, rng, source, target, shards_of, factor):
    owner, partner = [(jnp.arange(values.shape[dim]) // (values.shape[dim] // shards_of)).reshape([-1 if axis == dim else 1 for axis in range(values.ndim)]) for dim in (source, target)]
    chosen = jax.random.permutation(rng, shards_of)[partner]
    strong = (owner == chosen) | (owner == (partner + shards_of // 2) % shards_of)
    return jnp.where(strong, factor * values, values)


def block_scale(own_key, dims, split, least, largest):
    loudness = 1.0
    for dim, parts in split:
        heights = jax.random.uniform(jax.random.fold_in(jax.random.fold_in(own_key, 6), dim), (parts,), jnp.float32, least / len(split), largest / len(split))
        loudness = loudness * jnp.repeat(jnp.exp(heights), dims[dim] // parts).reshape((-1,) + (1,) * (len(dims) - 1 - dim))
    return loudness


def noise(rng, shape, spread, reach, split=(), kind=jnp.bfloat16):
    result = spread * jax.random.normal(rng, shape, jnp.float32)
    if split:
        result = result * block_scale(rng, shape, split, -0.22, 0.18)
    return jnp.clip(result, -reach, reach).astype(kind)


def heavy_noise(stream_key, dims, scale, limit, cuts, heavy, kind=jnp.bfloat16):
    array = scale * jax.random.normal(stream_key, dims, jnp.float32)
    if cuts:
        array = array * block_scale(stream_key, dims, cuts, -0.22, 0.18)
    return jnp.clip(with_spikes(array, jax.random.fold_in(stream_key, 3), *heavy), -limit, limit).astype(kind)


def setup_inputs(seed: int = 0, part: int = 0) -> dict:
    streams_of = jax.random.split(jax.random.key(seed), 9)
    own_keys = jax.random.split(jax.random.fold_in(streams_of[8], part), 9)
    activations = noise(own_keys[0], (LAYERS, TOKENS, D), 1.0, 6.0, ((0, 2), (1, 2), (2, 4)))
    cotangents = noise(own_keys[1], (LAYERS, TOKENS, D), 1.0, 6.0, ((0, 2), (1, 8)))
    out_weight = noise(streams_of[2], (LAYERS, D, D), D ** -0.5, 0.0625, ((0, 2), (1, 4), (2, 2)))
    in_sketch = noise(streams_of[3], (LAYERS, RANK, D), (D // 16) ** -0.5, 0.25, ((0, 2), (2, 4)))
    out_sketch = noise(streams_of[4], (LAYERS, RANK, D), (D // 16) ** -0.5, 0.25, ((0, 2),))
    queries = heavy_noise(streams_of[5], (LAYERS, QUERIES, FEAT), (LAYERS * FEAT) ** -0.5, 0.09375, ((0, 2), (1, 2), (2, 4)), (2, 1, 4, 2.0))
    lengths = touch_ends(jax.random.randint(own_keys[6], (EXAMPLES,), LEN // 2, LEN + 1), jax.random.fold_in(own_keys[6], 1), LEN // 2, LEN).astype(jnp.int32)
    store_order = jax.random.permutation(own_keys[7], EXAMPLES).astype(jnp.int32)
    return dict(activations=activations, cotangents=cotangents, out_weight=out_weight, in_sketch=in_sketch, out_sketch=out_sketch, queries=queries, lengths=lengths, store_order=store_order)


def reference(activations, cotangents, out_weight, in_sketch, out_sketch, queries, lengths, store_order):
    token_count = cotangents.shape[1]
    example_count = lengths.shape[0]
    token_ids = jnp.arange(token_count, dtype=jnp.int32)
    example_of = token_ids // LEN
    position = token_ids % LEN
    row_limit = jnp.take(lengths, example_of)
    loss_mask = (position < row_limit).astype(jnp.bfloat16)
    grad_list = []
    sketch_list = []
    for layer_idx in range(LAY_DEV * N_PIPE):
        masked = cotangents[layer_idx] * loss_mask[:, None]
        grad_list.append(jnp.dot(masked, out_weight[layer_idx].T, preferred_element_type=jnp.float32).astype(jnp.bfloat16))
        out_proj = jnp.dot(masked, out_sketch[layer_idx].T, preferred_element_type=jnp.float32).astype(jnp.bfloat16)
        in_proj = jnp.dot(activations[layer_idx], in_sketch[layer_idx].T, preferred_element_type=jnp.float32)
        out_rows = out_proj.astype(jnp.float32).reshape(example_count, LEN, RANK)
        in_rows = in_proj.reshape(example_count, LEN, RANK)
        outer_sum = jnp.einsum("etr,etc->erc", out_rows, in_rows, precision=lax.Precision.HIGHEST)
        outer_sum = outer_sum.reshape(example_count, RANK * RANK) / lengths.astype(jnp.float32)[:, None]
        sketch_list.append(outer_sum.astype(jnp.bfloat16))
    sketches = jnp.stack(sketch_list)
    sketch_store = jnp.take(sketches, store_order, axis=1)
    scores = jnp.einsum("lef,lqf->eq", sketches.astype(jnp.float32), queries.astype(jnp.float32), precision=lax.Precision.HIGHEST)
    return jnp.stack(grad_list), sketch_store, scores
```

```python
import jax
import jax.numpy as jnp
from jax import lax
from jax.sharding import PartitionSpec as P

RANK = 64
LEN = 256
SEQ_DEV = 2
CHUNKS = 2


def line_plan(count):
    def partner(place, odd):
        other = place + 1 if (place % 2 == 0) != odd else place - 1
        return other if 0 <= other < count else None

    streams = []
    for first_odd in (False, True):
        held = list(range(count))
        steps = []
        for step in range(1, count):
            odd = first_odd ^ (step % 2 == 0)
            got = [None] * count
            pairs = []
            for place in range(count):
                other = partner(place, odd)
                if other is not None and held[other] is not None:
                    got[place] = held[other]
                    pairs.append((other, place))
            steps.append((pairs, got))
            held = got
        streams.append(steps)
    return streams


def masked_rows(lengths, first_token, rows):
    token = first_token + jnp.arange(rows, dtype=jnp.int32)
    example_of = token // LEN
    position = token % LEN
    example_ids = jnp.arange(lengths.shape[0], dtype=jnp.int32)
    limit = jnp.sum(
        jnp.where(example_of[:, None] == example_ids[None, :], lengths[None, :], 0), axis=1
    )
    return position < limit


def rotate_gather(value, axis, count):
    out = [value]
    for shift in range(1, count):
        out.append(lax.ppermute(value, axis, [((a + shift) % count, a) for a in range(count)]))
    return out


def per_device(
    activations, cotangents, out_weight, in_sketch, out_sketch, queries, lengths, store_order
):
    tensor_count = lax.axis_size("tensor")
    dp_count = lax.axis_size("dp")
    pipe_count = lax.axis_size("pipe")
    slab_rows = cotangents.shape[1]
    width = cotangents.shape[2]
    local_tokens = slab_rows * tensor_count
    example_count = lengths.shape[0]
    dp_index = lax.axis_index("dp")
    tensor_index = lax.axis_index("tensor")
    pipe_index = lax.axis_index("pipe")
    rows = cotangents[0]
    layer_weight = out_weight[0]
    features = layer_weight.shape[0]
    block = width // dp_count
    piece = block // CHUNKS

    def cut(owner, chunk):
        return lax.dynamic_slice_in_dim(rows, owner * block + chunk * piece, piece, 1)

    held = {}
    for chunk in range(CHUNKS):
        held[0, chunk] = cut(dp_index, chunk)
    for shift in range(1, dp_count):
        for chunk in range(CHUNKS):
            held[shift, chunk] = lax.ppermute(
                cut((dp_index + shift) % dp_count, chunk),
                "dp",
                [(a, (a + shift) % dp_count) for a in range(dp_count)],
            )

    plan = line_plan(tensor_count)
    streams = {}
    for key, value in held.items():
        for which, steps in enumerate(plan):
            moving = value
            for step, (pairs, _) in enumerate(steps, 1):
                if not pairs:
                    break
                moving = lax.ppermute(moving, "tensor", pairs)
                streams[key, which, step] = moving

    def blocks_of(which, step):
        return plan[which][step - 1][1]

    def slot(key, index):
        if index == 0:
            return held[key]
        first, second = (key, 0, index), (key, 1, tensor_count - index)
        if second not in streams:
            return streams[first]
        valid = jnp.array([b is not None for b in blocks_of(0, index)])[tensor_index]
        return jnp.where(valid, streams[first], streams[second])

    slab_of = [tensor_index]
    for index in range(1, tensor_count):
        table = []
        for place in range(tensor_count):
            first = blocks_of(0, index)[place]
            second = blocks_of(1, tensor_count - index)[place]
            table.append(first if first is not None else second)
        assert None not in table
        slab_of.append(jnp.array(table, dtype=jnp.int32)[tensor_index])

    def product(pieces):
        total = None
        for chunk, value in enumerate(pieces):
            part = lax.dot_general(
                value,
                layer_weight[:, chunk * piece : (chunk + 1) * piece],
                (((1,), (1,)), ((), ())),
                preferred_element_type=jnp.float32,
            )
            total = part if total is None else total + part
        return total

    act_grad = jnp.zeros((local_tokens, features), jnp.bfloat16)
    for index in range(tensor_count):
        total = product([slot((0, chunk), index) for chunk in range(CHUNKS)])
        for shift in range(1, dp_count):
            partial = product([slot((shift, chunk), index) for chunk in range(CHUNKS)])
            total = total + lax.ppermute(
                partial.astype(jnp.bfloat16),
                "dp",
                [(a, (a - shift) % dp_count) for a in range(dp_count)],
            ).astype(jnp.float32)
        keep = masked_rows(
            lengths, dp_index * local_tokens + slab_of[index] * slab_rows, slab_rows
        )
        slab = jnp.where(keep[:, None], total, 0.0).astype(jnp.bfloat16)
        act_grad = lax.dynamic_update_slice_in_dim(act_grad, slab, slab_of[index] * slab_rows, 0)

    own_keep = masked_rows(
        lengths, dp_index * local_tokens + tensor_index * slab_rows, slab_rows
    )
    own_proj = jnp.dot(rows, out_sketch[0].T, preferred_element_type=jnp.float32)
    own_proj = jnp.where(own_keep[:, None], own_proj, 0.0).astype(jnp.bfloat16)
    out_proj = jnp.zeros((local_tokens, RANK), jnp.bfloat16)
    for shift, value in enumerate(rotate_gather(own_proj, "tensor", tensor_count)):
        out_proj = lax.dynamic_update_slice_in_dim(
            out_proj, value, ((tensor_index + shift) % tensor_count) * slab_rows, 0
        )
    in_proj = jnp.dot(activations[0], in_sketch[0].T, preferred_element_type=jnp.float32)
    out_rows = out_proj.astype(jnp.float32).reshape(SEQ_DEV, LEN, RANK)
    in_rows = in_proj.reshape(SEQ_DEV, LEN, RANK)
    outer_sum = jnp.einsum("etr,etc->erc", out_rows, in_rows, precision=lax.Precision.HIGHEST)
    outer_sum = outer_sum.reshape(SEQ_DEV, RANK * RANK)
    share = RANK * RANK // tensor_count
    summed = lax.dynamic_slice_in_dim(outer_sum, tensor_index * share, share, 1)
    for shift in range(1, tensor_count):
        summed = summed + lax.ppermute(
            lax.dynamic_slice_in_dim(
                outer_sum, ((tensor_index + shift) % tensor_count) * share, share, 1
            ),
            "tensor",
            [(a, (a + shift) % tensor_count) for a in range(tensor_count)],
        )
    own_lengths = lax.dynamic_slice_in_dim(lengths, dp_index * SEQ_DEV, SEQ_DEV).astype(jnp.float32)
    own_sketch = (summed / own_lengths[:, None]).astype(jnp.bfloat16)
    all_sketch = jnp.zeros((example_count, share), jnp.bfloat16)
    for shift, value in enumerate(rotate_gather(own_sketch, "dp", dp_count)):
        all_sketch = lax.dynamic_update_slice_in_dim(
            all_sketch, value, ((dp_index + shift) % dp_count) * SEQ_DEV, 0
        )
    example_ids = jnp.arange(example_count, dtype=jnp.int32)
    own_order = lax.dynamic_slice_in_dim(store_order, dp_index * SEQ_DEV, SEQ_DEV)
    selector = (own_order[:, None] == example_ids[None, :]).astype(jnp.bfloat16)
    sketch_store = jnp.einsum(
        "re,ef->rf", selector, all_sketch, preferred_element_type=jnp.float32
    ).astype(jnp.bfloat16)
    partial_scores = jnp.einsum(
        "ef,qf->eq", all_sketch, queries[0], preferred_element_type=jnp.float32
    )
    parts = partial_scores.reshape(example_count, tensor_count, pipe_count, -1)
    parts = parts.transpose(2, 1, 0, 3)
    kept = lax.dynamic_index_in_dim(parts, pipe_index, 0, False)
    for shift in range(1, pipe_count):
        kept = kept + lax.ppermute(
            lax.dynamic_index_in_dim(parts, (pipe_index + shift) % pipe_count, 0, False),
            "pipe",
            [(a, (a + shift) % pipe_count) for a in range(pipe_count)],
        )
    scores = lax.dynamic_index_in_dim(kept, tensor_index, 0, False)
    for shift in range(1, tensor_count):
        scores = scores + lax.ppermute(
            lax.dynamic_index_in_dim(kept, (tensor_index + shift) % tensor_count, 0, False),
            "tensor",
            [(a, (a + shift) % tensor_count) for a in range(tensor_count)],
        )
    return (act_grad[None], sketch_store[None], scores)


def solution(mesh):
    placed = (
        P("pipe", ("groups", "dp"), "tensor"),
        P("pipe", ("groups", "dp", "tensor"), None),
        P("pipe", "tensor", "dp"),
        P("pipe", None, "tensor"),
        P("pipe", None, None),
        P("pipe", "dp", "tensor"),
        P("groups"),
        P("groups"),
    )
    return jax.shard_map(
        per_device,
        mesh=mesh,
        in_specs=placed,
        out_specs=(
            P("pipe", ("groups", "dp"), "tensor"),
            P("pipe", ("groups", "dp"), "tensor"),
            P("groups", ("dp", "tensor", "pipe")),
        ),
        check_vma=False,
    )
```
